32 devices in a mesh: seq: 8 (over z, core), ch: 4 (over y, x).
Axes of the slice: x: 2, y: 2, z: 4, core: 2. Of those that a mesh axis runs over, the one named last changes fastest.
Arguments:
- input_q: bfloat16 [4096, 8192], P('seq', 'ch'), may hold values from -6 to 6
- input_k: bfloat16 [4096, 8192], P('seq', 'ch'), may hold values from -6 to 6
- input_v: bfloat16 [4096, 8192], P('seq', 'ch'), may hold values from -6 to 6
- grad_out: bfloat16 [4096, 8192], P('seq', 'ch'), may hold values from -6 to 6
- short_filters: float32 [3, 3, 8192], P(None, None, 'ch'), may hold values from -3.5 to 3.5
- long_filter: float32 [128, 8192], P(None, 'ch'), may hold values from -0.5 to 0.5
- skip_gain: float32 [8192], P('ch'), may hold values from 0.5 to 1.5
Outputs:
- grad_input_q: bfloat16 [4096, 8192], P('seq', 'ch')
- grad_input_k: bfloat16 [4096, 8192], P('seq', 'ch')
- grad_input_v: bfloat16 [4096, 8192], P('seq', 'ch')
- grad_long: float32 [128, 8192], P('seq', 'ch')
- grad_short: float32 [3, 3, 8192], P(None, None, 'ch')
- grad_skip: float32 [8192], P('ch')
The draws below stay inside these ranges and needn't reach their ends.
All inputs are finite; a program needn't handle non-finite values.
Results may differ from the reference program's by a relative error of at most 0.001.
Values may be sent and summed in bfloat16 or wider, within the bound.
A program may use at most 128 MiB of HBM per device.

```python
import math
import jax
import jax.numpy as jnp
from jax import lax

D = 8192
TAPS = 3
FILT = 128
SEQ = 4096


def levels(stream_key, shape, shards, smallest, high):
    level, own = 1.0, jax.random.fold_in(stream_key, 6)
    for axis_at, shards_of in shards:
        draws = jnp.exp(jax.random.uniform(jax.random.fold_in(own, axis_at), (shards_of,), jnp.float32, smallest / len(shards), high / len(shards)))
        level = level * jnp.repeat(draws, shape[axis_at] // shards_of).reshape([-1 if axis == axis_at else 1 for axis in range(len(shape))])
    return level


def gaussian(key, dims, scale, limit, cuts=(), dtype=jnp.bfloat16):
    factor_of = levels(key, dims, cuts, -0.22, 0.18) if cuts else 1.0
    entries = jax.random.normal(key, dims, jnp.float32) * scale * factor_of
    return jnp.minimum(jnp.maximum(entries, -limit), limit).astype(dtype)


def setup_inputs(seed: int = 0) -> dict:
    arg_keys = jax.random.split(jax.random.key(seed), 8)
    return {
        "input_q": gaussian(arg_keys[0], (SEQ, D), 1.0, 6.0, ((0, 8), (1, 4))),
        "input_k": gaussian(arg_keys[1], (SEQ, D), 1.0, 6.0, ((0, 8), (1, 4))),
        "input_v": gaussian(arg_keys[2], (SEQ, D), 1.0, 6.0, ((0, 8), (1, 4))),
        "grad_out": gaussian(arg_keys[3], (SEQ, D), 1.0, 6.0, ((0, 8), (1, 4))),
        "short_filters": gaussian(arg_keys[4], (3, TAPS, D), TAPS ** -0.5, 3.5, ((2, 4),), jnp.float32),
        "long_filter": gaussian(arg_keys[5], (FILT, D), FILT ** -0.5, 0.5, ((1, 4),), jnp.float32),
        "skip_gain": jnp.clip(0.5 + 1.0 * jax.random.uniform(arg_keys[6], (D,), jnp.float32) ** levels(arg_keys[6], (D,), ((0, 4),), -0.2, 0.2), 0.5, 1.5),
    }


def one_block(packed):
    query_in, key_in, value_in, upstream, taps_w, filt, gain = packed
    length = query_in.shape[0]
    ntap = taps_w.shape[1]

    def short_conv(signal, weights):
        padded = jnp.pad(signal, ((ntap - 1, 0), (0, 0)))
        total = jnp.zeros_like(signal)
        for index in range(ntap):
            total = total + weights[index] * padded[ntap - 1 - index:ntap - 1 - index + length]
        return total

    def short_back(grad, weights, signal):
        grad_pad = jnp.pad(grad, ((0, ntap - 1), (0, 0)))
        sig_pad = jnp.pad(signal, ((ntap - 1, 0), (0, 0)))
        result = jnp.zeros_like(grad)
        rows_taps = []
        for index in range(ntap):
            result = result + weights[index] * grad_pad[index:index + length]
            rows_taps.append(jnp.sum(grad * sig_pad[ntap - 1 - index:ntap - 1 - index + length], axis=0))
        return result, jnp.stack(rows_taps)

    q_sig = query_in.astype(jnp.float32)
    k_sig = key_in.astype(jnp.float32)
    v_sig = value_in.astype(jnp.float32)
    dy_sig = upstream.astype(jnp.float32)
    q_feat = short_conv(q_sig, taps_w[0])
    k_feat = short_conv(k_sig, taps_w[1])
    v_feat = short_conv(v_sig, taps_w[2])
    z_feat = k_feat * v_feat
    double = 2 * length
    spec_h = jnp.fft.rfft(filt, n=double, axis=0)
    spec_z = jnp.fft.rfft(z_feat, n=double, axis=0)
    s_feat = jnp.fft.irfft(spec_z * spec_h, n=double, axis=0)[:length].astype(jnp.float32) + gain * z_feat
    grad_q = dy_sig * s_feat
    grad_s = dy_sig * q_feat
    spec_s = jnp.fft.rfft(grad_s, n=double, axis=0)
    grad_z = jnp.fft.irfft(spec_s * jnp.conj(spec_h), n=double, axis=0)[:length].astype(jnp.float32) + gain * grad_s
    grad_k = grad_z * v_feat
    grad_v = grad_z * k_feat
    grad_filt = jnp.fft.irfft(spec_s * jnp.conj(spec_z), n=double, axis=0)[:filt.shape[0]].astype(jnp.float32)
    grad_gain = jnp.sum(grad_s * z_feat, axis=0)
    back_q, taps_q = short_back(grad_q, taps_w[0], q_sig)
    back_k, taps_k = short_back(grad_k, taps_w[1], k_sig)
    back_v, taps_v = short_back(grad_v, taps_w[2], v_sig)
    return (back_q.astype(jnp.bfloat16), back_k.astype(jnp.bfloat16), back_v.astype(jnp.bfloat16),
            grad_filt, jnp.stack([taps_q, taps_k, taps_v]), grad_gain)


def reference(input_q, input_k, input_v, grad_out, short_filters, long_filter, skip_gain):
    length, width = input_q.shape
    block = math.gcd(width, 512)
    count = width // block

    def split(array):
        return array.reshape(array.shape[0], count, block).transpose(1, 0, 2)

    def merge(array):
        return array.transpose(1, 0, 2).reshape(array.shape[1], width)

    packed = (split(input_q), split(input_k), split(input_v), split(grad_out),
              short_filters.reshape(3, short_filters.shape[1], count, block).transpose(2, 0, 1, 3),
              split(long_filter), skip_gain.reshape(count, block))
    back_q, back_k, back_v, grad_filt, grad_taps, grad_gain = lax.map(one_block, packed)
    grad_taps = grad_taps.transpose(1, 2, 0, 3).reshape(3, short_filters.shape[1], width)
    return (merge(back_q), merge(back_k), merge(back_v), merge(grad_filt), grad_taps, grad_gain.reshape(width))
```

```python
import functools

import jax
import jax.numpy as jnp
import numpy as np
from jax import lax
from jax.experimental import pallas as pl
from jax.experimental.pallas import tpu as pltpu
from jax.sharding import PartitionSpec as P

F32 = jnp.float32
BF16 = jnp.bfloat16
ROWS = 16


def shifted(value, axis, by):
    size = lax.axis_size(axis)
    pairs = [(i, i + by) for i in range(size) if 0 <= i + by < size]
    return lax.ppermute(value, axis, pairs)


def transforms(span):
    freq = np.concatenate([np.arange(0, span, 2), np.arange(1, span, 2)]) + 0.5
    angle = np.pi * np.outer(freq, np.arange(span)) / span
    fwd = np.concatenate([np.cos(angle), -np.sin(angle)], 0)
    inv = fwd.T / span

    def halves(mat):
        mat = mat.astype(np.float32)
        high = mat.astype(jnp.bfloat16)
        low = (mat - high.astype(np.float32)).astype(jnp.bfloat16)
        return high, low

    fh, fl = halves(fwd)
    ih, il = halves(inv)
    return (
        np.concatenate([fh, fh], 1),
        fl,
        ih,
        il,
    )


def split(value):
    high = value.astype(BF16)
    low = (value - high.astype(F32)).astype(BF16)
    return high, low


def down(window, by, rows):
    return pltpu.roll(window, by, 0)[8 : 8 + rows]


def up(window, by, rows):
    return pltpu.roll(window, rows + 8 - by, 0)[:rows]


def kernel(
    length, span, ntap, pad,
    q_ref, k_ref, v_ref, g_ref, kp_ref, vp_ref, qp_ref, qn_ref, gn_ref, kn_ref, vn_ref,
    sf_ref, lf_ref, hr_ref, gain_ref, fh_ref, fl_ref, ih_ref, il_ref,
    bq_ref, bk_ref, bv_ref, part_ref,
    qx, kx, vx, gx, kf, vf, zf, gs, zs, gss, zw, gw, hw, acc, sx, gz, prod,
):
    width = q_ref.shape[1]
    half = span // 2
    nblk = length // span
    big = span + pad
    kx[:big] = kp_ref[...].astype(F32)
    kx[big : big + length] = k_ref[...].astype(F32)
    kx[big + length :] = kn_ref[...].astype(F32)
    vx[:big] = vp_ref[...].astype(F32)
    vx[big : big + length] = v_ref[...].astype(F32)
    vx[big + length :] = vn_ref[...].astype(F32)
    qx[:pad] = qp_ref[...].astype(F32)
    qx[pad : pad + length] = q_ref[...].astype(F32)
    qx[pad + length :] = qn_ref[...].astype(F32)
    gx[:length] = g_ref[...].astype(F32)
    gx[length:] = gn_ref[...].astype(F32)

    def taps(which):
        return [jnp.broadcast_to(sf_ref[which, i : i + 1, :], (ROWS, width)) for i in range(ntap)]

    def conv(ref, row, weights):
        window = ref[pl.ds(row - 8, ROWS + 8), :]
        total = weights[0] * window[8:]
        for i in range(1, ntap):
            total = total + weights[i] * down(window, i, ROWS)
        return total

    wk, wv, wq = taps(1), taps(2), taps(0)
    per = span // ROWS

    def make_z(c, _):
        row = pl.multiple_of(c * ROWS, ROWS)
        a = conv(kx, row + pad, wk)
        b = conv(vx, row + pad, wv)
        z = a * b
        kf[pl.ds(row, ROWS), :] = a
        vf[pl.ds(row, ROWS), :] = b
        zf[pl.ds(row, ROWS), :] = z
        return 0

    lax.fori_loop(0, (span + length + pad) // ROWS, make_z, 0, unroll=2)

    def make_g(c, _):
        row = pl.multiple_of(c * ROWS, ROWS)
        gs[pl.ds(row, ROWS), :] = gx[pl.ds(row, ROWS), :] * conv(qx, row + pad, wq)
        return 0

    lax.fori_loop(0, (length + span + pad) // ROWS, make_g, 0, unroll=2)

    def forward(block, out):
        high, low = split(block)
        stack = jnp.concatenate([high, low], 0)
        out[...] = jnp.dot(fh_ref[...], stack, preferred_element_type=F32) + jnp.dot(
            fl_ref[...], high, preferred_element_type=F32
        )

    def inverse(out):
        out[...] = (
            jnp.dot(ih_ref[...], prod[0], preferred_element_type=F32)
            + jnp.dot(ih_ref[...], prod[1], preferred_element_type=F32)
            + jnp.dot(il_ref[...], prod[0], preferred_element_type=F32)
        )

    first = lax.broadcasted_iota(jnp.int32, (span, width), 0) == 0
    forward(lf_ref[...] + jnp.where(first, gain_ref[...], 0.0), hw)

    def fwd_both(b, _):
        row = pl.multiple_of(b * span, span)
        forward(zf[pl.ds(row, span), :], zw.at[b])
        forward(gs[pl.ds(row, span), :], gw.at[b])
        return 0

    lax.fori_loop(0, nblk + 1, fwd_both, 0)
    acc[...] = jnp.zeros_like(acc)

    def point(b, _):
        row = pl.multiple_of(b * span, span)
        for c in range(span // ROWS):
            sign = 1 if c * ROWS < half else -1
            re = slice(c * ROWS, (c + 1) * ROWS)
            im = slice(span + c * ROWS, span + (c + 1) * ROWS)
            hr, hi = hw[re], hw[im]
            if sign > 0:
                yr = zw[b + 1, re] - zw[b, im]
                yi = zw[b + 1, im] + zw[b, re]
            else:
                yr = zw[b + 1, re] + zw[b, im]
                yi = zw[b + 1, im] - zw[b, re]
            gr, gi = gw[b, re], gw[b, im]
            ph, plo = split(yr * hr - yi * hi)
            prod[0, re] = ph
            prod[1, re] = plo
            ph, plo = split(yr * hi + yi * hr)
            prod[0, im] = ph
            prod[1, im] = plo
            acc[re] += gr * yr + gi * yi
            acc[im] += gi * yr - gr * yi
        inverse(sx.at[pl.ds(row, span)])
        for c in range(span // ROWS):
            sign = 1 if c * ROWS < half else -1
            re = slice(c * ROWS, (c + 1) * ROWS)
            im = slice(span + c * ROWS, span + (c + 1) * ROWS)
            hr, hi = hw[re], hw[im]
            if sign > 0:
                yr = gw[b, re] + gw[b + 1, im]
                yi = gw[b, im] - gw[b + 1, re]
            else:
                yr = gw[b, re] - gw[b + 1, im]
                yi = gw[b, im] + gw[b + 1, re]
            ph, plo = split(yr * hr + yi * hi)
            prod[0, re] = ph
            prod[1, re] = plo
            ph, plo = split(yi * hr - yr * hi)
            prod[0, im] = ph
            prod[1, im] = plo
        inverse(gz.at[pl.ds(row, span)])
        return 0

    lax.fori_loop(0, nblk, point, 0)
    for c in range(span // ROWS):
        for start in (0, span):
            rows = slice(start + c * ROWS, start + (c + 1) * ROWS)
            ph, plo = split(acc[rows])
            prod[0, rows] = ph
            prod[1, rows] = plo
    inverse(part_ref.at[:span])

    taps_h = lf_ref[...]
    back_h = hr_ref[...]
    gain = gain_ref[...]
    line = lax.broadcasted_iota(jnp.int32, (8, width), 0)
    edge_s = jnp.zeros((8, width), F32)
    edge_z = jnp.zeros((8, width), F32)
    for i in range(ntap - 1):
        zrow = zf[length + span + i : length + span + i + 1, :]
        grow = gs[length + i : length + i + 1, :]
        win = zf[length + i + 1 : length + i + 1 + span, :]
        value = jnp.sum(win * back_h, axis=0, keepdims=True) + gain * zrow
        edge_s = jnp.where(line == i, value, edge_s)
        win = gs[length + i : length + i + span, :]
        value = jnp.sum(win * taps_h, axis=0, keepdims=True) + gain * grow
        edge_z = jnp.where(line == i, value, edge_z)
    eq = gx[length : length + 8] * edge_s
    ek = edge_z * vf[length + span : length + span + 8]
    ev = edge_z * kf[length + span : length + span + 8]

    def back(grad, after, weights, out_ref, row, own, sums):
        window = jnp.concatenate([grad, after], 0)
        total = weights[0] * grad
        new = [sums[0] + fold(grad * own)]
        for i in range(1, ntap):
            later = up(window, i, ROWS)
            total = total + weights[i] * later
            new.append(sums[i] + fold(later * own))
        out_ref[pl.ds(row, ROWS), :] = total.astype(BF16)
        return grad[:8], new

    def fold(value):
        total = value[:8]
        for r in range(8, ROWS, 8):
            total = total + value[r : r + 8]
        return total

    steps = length // ROWS

    def last(c, carry):
        after, sums = carry
        row = pl.multiple_of((steps - 1 - c) * ROWS, ROWS)
        gzc = gz[pl.ds(row, ROWS), :]
        gq = gx[pl.ds(row, ROWS), :] * sx[pl.ds(row, ROWS), :]
        gk = gzc * vf[pl.ds(row + span, ROWS), :]
        gv = gzc * kf[pl.ds(row + span, ROWS), :]
        aq, s0 = back(gq, after[0], wq, bq_ref, row, qx[pl.ds(row + pad, ROWS), :], sums[0])
        ak, s1 = back(gk, after[1], wk, bk_ref, row, kx[pl.ds(row + big, ROWS), :], sums[1])
        av, s2 = back(gv, after[2], wv, bv_ref, row, vx[pl.ds(row + big, ROWS), :], sums[2])
        return (aq, ak, av), (s0, s1, s2)

    zero = [jnp.zeros((8, width), F32) for _ in range(ntap)]
    _, sums = lax.fori_loop(0, steps, last, ((eq, ek, ev), (zero, zero, zero)), unroll=2)
    rows = [jnp.sum(sums[w][i], axis=0, keepdims=True) for w in range(3) for i in range(ntap)]
    rows.append(part_ref[0:1, :])
    extra = part_ref.shape[0] - span - len(rows)
    part_ref[span:] = jnp.concatenate(rows + [jnp.zeros((extra, width), F32)], 0)


def body(input_q, input_k, input_v, grad_out, short_filters, long_filter, skip_gain):
    length, channels = input_q.shape
    ntap = short_filters.shape[1]
    span = long_filter.shape[0]
    pad = 16
    big = span + pad
    width = min(256, channels)
    kp = shifted(input_k[length - big :], "seq", 1)
    vp = shifted(input_v[length - big :], "seq", 1)
    qp = shifted(input_q[length - pad :], "seq", 1)
    qn = shifted(input_q[:big], "seq", -1)
    gn = shifted(grad_out[:big], "seq", -1)
    kn = shifted(input_k[:pad], "seq", -1)
    vn = shifted(input_v[:pad], "seq", -1)
    mats = [jnp.asarray(m) for m in transforms(span)]
    nblk = length // span

    def tile(rows):
        return pl.BlockSpec((rows, width), lambda i: (0, i))

    def whole(mat):
        return pl.BlockSpec(mat.shape, lambda i: (0, 0))

    more = -(-(3 * ntap + 1) // 8) * 8
    cells = lambda rows: pltpu.VMEM((rows, width), F32)
    ext = length + big
    back_q, back_k, back_v, part = pl.pallas_call(
        functools.partial(kernel, length, span, ntap, pad),
        grid=(channels // width,),
        out_shape=(
            jax.ShapeDtypeStruct((length, channels), BF16),
            jax.ShapeDtypeStruct((length, channels), BF16),
            jax.ShapeDtypeStruct((length, channels), BF16),
            jax.ShapeDtypeStruct((span + more, channels), F32),
        ),
        in_specs=[tile(length)] * 4
        + [tile(big), tile(big), tile(pad), tile(big), tile(big), tile(pad), tile(pad)]
        + [pl.BlockSpec((3, ntap, width), lambda i: (0, 0, i)), tile(span), tile(span), tile(1)]
        + [whole(m) for m in mats],
        out_specs=(tile(length), tile(length), tile(length), tile(span + more)),
        scratch_shapes=[
            cells(ext + pad), cells(ext + pad), cells(ext + pad), cells(ext),
            cells(ext), cells(ext), cells(ext), cells(ext),
            cells(8), cells(8),
            pltpu.VMEM((nblk + 1, 2 * span, width), F32),
            pltpu.VMEM((nblk + 1, 2 * span, width), F32),
            cells(2 * span), cells(2 * span), cells(length), cells(length),
            pltpu.VMEM((2, 2 * span, width), BF16),
        ],
        compiler_params=pltpu.CompilerParams(
            dimension_semantics=("arbitrary",), vmem_limit_bytes=56 * 1024 * 1024
        ),
        name="hyena_back",
    )(
        input_q, input_k, input_v, grad_out, kp, vp, qp, qn, gn, kn, vn,
        short_filters, long_filter, long_filter[::-1], skip_gain[None], *mats,
    )
    grad_filt = lax.psum_scatter(part[:span], "seq", scatter_dimension=0, tiled=True)
    small = lax.psum(part[span:], "seq")
    grad_taps = small[: 3 * ntap].reshape(3, ntap, channels)
    return (back_q, back_k, back_v, grad_filt, grad_taps, small[3 * ntap])


def solution(mesh):
    return jax.shard_map(
        body,
        mesh=mesh,
        in_specs=(
            P("seq", "ch"),
            P("seq", "ch"),
            P("seq", "ch"),
            P("seq", "ch"),
            P(None, None, "ch"),
            P(None, "ch"),
            P("ch"),
        ),
        out_specs=(
            P("seq", "ch"),
            P("seq", "ch"),
            P("seq", "ch"),
            P("seq", "ch"),
            P(None, None, "ch"),
            P("ch"),
        ),
        check_vma=False,
    )
```

```python
import functools

import jax
import jax.numpy as jnp
import numpy as np
from jax import lax
from jax.experimental import pallas as pl
from jax.experimental.pallas import tpu as pltpu
from jax.sharding import PartitionSpec as P

F32 = jnp.float32
BF16 = jnp.bfloat16
ROWS = 16


def transforms(span):
    freq = np.concatenate([np.arange(0, span, 2), np.arange(1, span, 2)]) + 0.5
    angle = np.pi * np.outer(freq, np.arange(span)) / span
    fwd = np.concatenate([np.cos(angle), -np.sin(angle)], 0)
    inv = fwd.T / span

    def halves(mat):
        mat = mat.astype(np.float32)
        high = mat.astype(jnp.bfloat16)
        low = (mat - high.astype(np.float32)).astype(jnp.bfloat16)
        return high, low

    fh, fl = halves(fwd)
    ih, il = halves(inv)
    return (
        np.concatenate([fh, fh], 1),
        fl,
        ih,
        il,
        np.concatenate([np.eye(span)[::-1]] * 2, 1).astype(jnp.bfloat16),
    )


def split(value):
    high = value.astype(BF16)
    low = (value - high.astype(F32)).astype(BF16)
    return high, low


def down(window, by, rows):
    return pltpu.roll(window, by, 0)[8 : 8 + rows]


def up(window, by, rows):
    return pltpu.roll(window, rows + 8 - by, 0)[:rows]


def remote(src, dst, send, recv, target):
    return pltpu.make_async_remote_copy(
        src_ref=src,
        dst_ref=dst,
        send_sem=send,
        recv_sem=recv,
        device_id={"seq": target},
        device_id_type=pl.DeviceIdType.MESH,
    )


def kernel(
    size, length, span, ntap, pad,
    q_ref, k_ref, v_ref, g_ref, q_all, k_all, v_all, g_all,
    sf_ref, lf_ref, gain_ref, fh_ref, fl_ref, ih_ref, il_ref, flip_ref,
    bq_ref, bk_ref, bv_ref, filt_ref, taps_ref, skip_ref,
    qx, kx, vx, gx, kf, vf, zf, gs, zw, gw, hw, acc, sx, gz, prod, part,
    kp_all, vp_all, qp_all, qn_all, gn_all, kn_all, vn_all,
    mine, theirs, chip, others,
    halo_send, halo_recv, pair_send, pair_recv, chip_send, chip_recv,
):
    width = q_ref.shape[1]
    half = span // 2
    nblk = length // span
    big = span + pad
    tile = pl.program_id(0)
    tiles = kp_all.shape[0]
    chips = size // 2
    block = span // size
    me = lax.axis_index("seq")
    core = lax.rem(me, 2)
    place = me // 2
    partner = me + 1 - 2 * core

    def to_next(t):
        cols = pl.ds(pl.multiple_of(t * width, width), width)
        target = lax.rem(me + 1, size)
        parts = ((k_all, big, kp_all), (v_all, big, vp_all), (q_all, pad, qp_all))
        return [
            remote(src.at[pl.ds(length - rows, rows), cols], dst.at[t], halo_send.at[t, j], halo_recv.at[t, j], target)
            for j, (src, rows, dst) in enumerate(parts)
        ]

    def to_prev(t):
        cols = pl.ds(pl.multiple_of(t * width, width), width)
        target = lax.rem(me + size - 1, size)
        parts = ((q_all, big, qn_all), (g_all, big, gn_all), (k_all, pad, kn_all), (v_all, pad, vn_all))
        return [
            remote(src.at[pl.ds(0, rows), cols], dst.at[t], halo_send.at[t, 3 + j], halo_recv.at[t, 3 + j], target)
            for j, (src, rows, dst) in enumerate(parts)
        ]

    def pair_copy(t):
        return remote(mine.at[t, 1 - core], theirs.at[t], pair_send.at[t], pair_recv.at[t], partner)

    def chip_copy(t, d):
        there = lax.rem(place + d, chips)
        return remote(chip.at[t, there], others.at[t, d], chip_send.at[t, d], chip_recv.at[t, d], there * 2 + core)

    @pl.when(tile == 0)
    def _():
        barrier = pltpu.get_barrier_semaphore()
        for d in range(1, size):
            pl.semaphore_signal(
                barrier, inc=1, device_id={"seq": lax.rem(me + d, size)}, device_id_type=pl.DeviceIdType.MESH
            )
        pl.semaphore_wait(barrier, size - 1)

        def send(t, _):
            @pl.when(me < size - 1)
            def _():
                for copy in to_next(t):
                    copy.start()

            @pl.when(me > 0)
            def _():
                for copy in to_prev(t):
                    copy.start()

            return 0

        lax.fori_loop(0, tiles, send, 0)

        @pl.when(me == 0)
        def _():
            for ref in (kp_all, vp_all, qp_all):
                ref[...] = jnp.zeros_like(ref)

        @pl.when(me == size - 1)
        def _():
            for ref in (qn_all, gn_all, kn_all, vn_all):
                ref[...] = jnp.zeros_like(ref)

    @pl.when(me > 0)
    def _():
        for copy in to_next(tile):
            copy.wait_recv()

    @pl.when(me < size - 1)
    def _():
        for copy in to_prev(tile):
            copy.wait_recv()

    kp_ref, vp_ref, qp_ref = kp_all.at[tile], vp_all.at[tile], qp_all.at[tile]
    qn_ref, gn_ref, kn_ref, vn_ref = qn_all.at[tile], gn_all.at[tile], kn_all.at[tile], vn_all.at[tile]

    def join_chip(t):
        pair_copy(t).wait_recv()
        total = mine[t, core] + theirs[t]
        chip[t] = total
        others[t, 0] = mine[t, core, place] + theirs[t, place]
        for d in range(1, chips):
            chip_copy(t, d).start()

    kx[:big] = kp_ref[...].astype(F32)
    kx[big : big + length] = k_ref[...].astype(F32)
    kx[big + length :] = kn_ref[...].astype(F32)
    vx[:big] = vp_ref[...].astype(F32)
    vx[big : big + length] = v_ref[...].astype(F32)
    vx[big + length :] = vn_ref[...].astype(F32)
    qx[:pad] = qp_ref[...].astype(F32)
    qx[pad : pad + length] = q_ref[...].astype(F32)
    qx[pad + length :] = qn_ref[...].astype(F32)
    gx[:length] = g_ref[...].astype(F32)
    gx[length:] = gn_ref[...].astype(F32)

    def taps(which):
        return [jnp.broadcast_to(sf_ref[which, i : i + 1, :], (ROWS, width)) for i in range(ntap)]

    def conv(ref, row, weights):
        window = ref[pl.ds(row - 8, ROWS + 8), :]
        total = weights[0] * window[8:]
        for i in range(1, ntap):
            total = total + weights[i] * down(window, i, ROWS)
        return total

    wk, wv, wq = taps(1), taps(2), taps(0)
    per = span // ROWS

    def make_z(c, _):
        row = pl.multiple_of(c * ROWS, ROWS)
        a = conv(kx, row + pad, wk)
        b = conv(vx, row + pad, wv)
        z = a * b
        kf[pl.ds(row, ROWS), :] = a
        vf[pl.ds(row, ROWS), :] = b
        zf[pl.ds(row, ROWS), :] = z
        return 0

    lax.fori_loop(0, (span + length + pad) // ROWS, make_z, 0, unroll=2)

    def make_g(c, _):
        row = pl.multiple_of(c * ROWS, ROWS)
        gs[pl.ds(row, ROWS), :] = gx[pl.ds(row, ROWS), :] * conv(qx, row + pad, wq)
        return 0

    lax.fori_loop(0, (length + span + pad) // ROWS, make_g, 0, unroll=2)

    def forward(block, out):
        high, low = split(block)
        stack = jnp.concatenate([high, low], 0)
        out[...] = jnp.dot(fh_ref[...], stack, preferred_element_type=F32) + jnp.dot(
            fl_ref[...], high, preferred_element_type=F32
        )

    def inverse(out):
        out[...] = (
            jnp.dot(ih_ref[...], prod[0], preferred_element_type=F32)
            + jnp.dot(ih_ref[...], prod[1], preferred_element_type=F32)
            + jnp.dot(il_ref[...], prod[0], preferred_element_type=F32)
        )

    first = lax.broadcasted_iota(jnp.int32, (span, width), 0) == 0
    forward(lf_ref[...] + jnp.where(first, gain_ref[...], 0.0), hw)

    def fwd_both(b, _):
        row = pl.multiple_of(b * span, span)
        forward(zf[pl.ds(row, span), :], zw.at[b])
        forward(gs[pl.ds(row, span), :], gw.at[b])
        return 0

    lax.fori_loop(0, nblk + 1, fwd_both, 0)
    acc[...] = jnp.zeros_like(acc)

    @pl.when(tile > 0)
    def _():
        join_chip(tile - 1)

    def point(b, _):
        row = pl.multiple_of(b * span, span)
        for c in range(span // ROWS):
            sign = 1 if c * ROWS < half else -1
            re = slice(c * ROWS, (c + 1) * ROWS)
            im = slice(span + c * ROWS, span + (c + 1) * ROWS)
            hr, hi = hw[re], hw[im]
            if sign > 0:
                yr = zw[b + 1, re] - zw[b, im]
                yi = zw[b + 1, im] + zw[b, re]
            else:
                yr = zw[b + 1, re] + zw[b, im]
                yi = zw[b + 1, im] - zw[b, re]
            gr, gi = gw[b, re], gw[b, im]
            ph, plo = split(yr * hr - yi * hi)
            prod[0, re] = ph
            prod[1, re] = plo
            ph, plo = split(yr * hi + yi * hr)
            prod[0, im] = ph
            prod[1, im] = plo
            acc[re] += gr * yr + gi * yi
            acc[im] += gi * yr - gr * yi
        inverse(sx.at[pl.ds(row, span)])
        for c in range(span // ROWS):
            sign = 1 if c * ROWS < half else -1
            re = slice(c * ROWS, (c + 1) * ROWS)
            im = slice(span + c * ROWS, span + (c + 1) * ROWS)
            hr, hi = hw[re], hw[im]
            if sign > 0:
                yr = gw[b, re] + gw[b + 1, im]
                yi = gw[b, im] - gw[b + 1, re]
            else:
                yr = gw[b, re] - gw[b + 1, im]
                yi = gw[b, im] + gw[b + 1, re]
            ph, plo = split(yr * hr + yi * hi)
            prod[0, re] = ph
            prod[1, re] = plo
            ph, plo = split(yi * hr - yr * hi)
            prod[0, im] = ph
            prod[1, im] = plo
        inverse(gz.at[pl.ds(row, span)])
        return 0

    lax.fori_loop(0, nblk, point, 0)
    for c in range(span // ROWS):
        for start in (0, span):
            rows = slice(start + c * ROWS, start + (c + 1) * ROWS)
            ph, plo = split(acc[rows])
            prod[0, rows] = ph
            prod[1, rows] = plo
    inverse(part)

    taps_h = lf_ref[...]
    back_h = jnp.dot(flip_ref[...], jnp.concatenate(split(taps_h), 0), preferred_element_type=F32)
    gain = gain_ref[...]
    line = lax.broadcasted_iota(jnp.int32, (8, width), 0)
    edge_s = jnp.zeros((8, width), F32)
    edge_z = jnp.zeros((8, width), F32)
    for i in range(ntap - 1):
        zrow = zf[length + span + i : length + span + i + 1, :]
        grow = gs[length + i : length + i + 1, :]
        win = zf[length + i + 1 : length + i + 1 + span, :]
        value = jnp.sum(win * back_h, axis=0, keepdims=True) + gain * zrow
        edge_s = jnp.where(line == i, value, edge_s)
        win = gs[length + i : length + i + span, :]
        value = jnp.sum(win * taps_h, axis=0, keepdims=True) + gain * grow
        edge_z = jnp.where(line == i, value, edge_z)
    eq = gx[length : length + 8] * edge_s
    ek = edge_z * vf[length + span : length + span + 8]
    ev = edge_z * kf[length + span : length + span + 8]

    def back(grad, after, weights, out_ref, row, own, sums):
        window = jnp.concatenate([grad, after], 0)
        total = weights[0] * grad
        new = [sums[0] + fold(grad * own)]
        for i in range(1, ntap):
            later = up(window, i, ROWS)
            total = total + weights[i] * later
            new.append(sums[i] + fold(later * own))
        out_ref[pl.ds(row, ROWS), :] = total.astype(BF16)
        return grad[:8], new

    def fold(value):
        total = value[:8]
        for r in range(8, ROWS, 8):
            total = total + value[r : r + 8]
        return total

    steps = length // ROWS

    def last(c, carry):
        after, sums = carry
        row = pl.multiple_of((steps - 1 - c) * ROWS, ROWS)
        gzc = gz[pl.ds(row, ROWS), :]
        gq = gx[pl.ds(row, ROWS), :] * sx[pl.ds(row, ROWS), :]
        gk = gzc * vf[pl.ds(row + span, ROWS), :]
        gv = gzc * kf[pl.ds(row + span, ROWS), :]
        aq, s0 = back(gq, after[0], wq, bq_ref, row, qx[pl.ds(row + pad, ROWS), :], sums[0])
        ak, s1 = back(gk, after[1], wk, bk_ref, row, kx[pl.ds(row + big, ROWS), :], sums[1])
        av, s2 = back(gv, after[2], wv, bv_ref, row, vx[pl.ds(row + big, ROWS), :], sums[2])
        return (aq, ak, av), (s0, s1, s2)

    zero = [jnp.zeros((8, width), F32) for _ in range(ntap)]
    _, sums = lax.fori_loop(0, steps, last, ((eq, ek, ev), (zero, zero, zero)), unroll=2)
    rows = [jnp.sum(sums[w][i], axis=0, keepdims=True) for w in range(3) for i in range(ntap)]
    rows.append(part[0:1, :])
    small = jnp.concatenate(rows + [jnp.zeros((pad - len(rows), width), F32)], 0)
    for d in range(size):
        mine[tile, d % 2, d // 2, :block] = part[d * block : (d + 1) * block]
        mine[tile, d % 2, d // 2, block:] = small
    pair_copy(tile).start()

    @pl.when(tile == tiles - 1)
    def _():
        join_chip(tiles - 1)

        def finish(t, _):
            cols = pl.ds(pl.multiple_of(t * width, width), width)

            @pl.when(me < size - 1)
            def _():
                for copy in to_next(t):
                    copy.wait_send()

            @pl.when(me > 0)
            def _():
                for copy in to_prev(t):
                    copy.wait_send()

            pair_copy(t).wait_send()
            for d in range(1, chips):
                chip_copy(t, d).wait_send()
                chip_copy(t, d).wait_recv()
            total = others[t, place]
            for z in range(1, chips):
                total = total + others[t, lax.rem(place + chips - z, chips)]
            filt_ref[:, cols] = total[:block]
            for w in range(3):
                for i in range(ntap):
                    at = block + w * ntap + i
                    taps_ref[w, i : i + 1, cols] = total[at : at + 1]
            at = block + 3 * ntap
            skip_ref[:, cols] = total[at : at + 1]
            return 0

        lax.fori_loop(0, tiles, finish, 0)


def body(input_q, input_k, input_v, grad_out, short_filters, long_filter, skip_gain):
    length, channels = input_q.shape
    ntap = short_filters.shape[1]
    span = long_filter.shape[0]
    pad = 16
    big = span + pad
    width = min(256, channels)
    mats = [jnp.asarray(m) for m in transforms(span)]
    nblk = length // span

    def tile(rows):
        return pl.BlockSpec((rows, width), lambda i: (0, i))

    def whole(mat):
        return pl.BlockSpec(mat.shape, lambda i: (0, 0))

    size = lax.axis_size("seq")
    tiles = channels // width
    chips = size // 2
    block = span // size
    cells = lambda *rows: pltpu.VMEM((*rows, width), F32)
    edge = lambda rows: pltpu.VMEM((tiles, rows, width), BF16)
    ext = length + big
    full = pl.BlockSpec(memory_space=pl.ANY)
    out = jax.ShapeDtypeStruct((length, channels), BF16)
    back_q, back_k, back_v, grad_filt, grad_taps, grad_gain = pl.pallas_call(
        functools.partial(kernel, size, length, span, ntap, pad),
        grid=(tiles,),
        out_shape=(
            out, out, out,
            jax.ShapeDtypeStruct((block, channels), F32),
            jax.ShapeDtypeStruct((3, ntap, channels), F32),
            jax.ShapeDtypeStruct((1, channels), F32),
        ),
        in_specs=[tile(length)] * 4
        + [full] * 4
        + [pl.BlockSpec((3, ntap, width), lambda i: (0, 0, i)), tile(span), tile(1)]
        + [whole(m) for m in mats],
        out_specs=(
            tile(length), tile(length), tile(length),
            pl.BlockSpec((block, channels), lambda i: (0, 0)),
            pl.BlockSpec((3, ntap, channels), lambda i: (0, 0, 0)),
            pl.BlockSpec((1, channels), lambda i: (0, 0)),
        ),
        scratch_shapes=[
            cells(ext + pad), cells(ext + pad), cells(ext + pad), cells(ext),
            cells(ext), cells(ext), cells(ext), cells(ext),
            cells(nblk + 1, 2 * span), cells(nblk + 1, 2 * span),
            cells(2 * span), cells(2 * span), cells(length), cells(length),
            pltpu.VMEM((2, 2 * span, width), BF16), cells(span),
            edge(big), edge(big), edge(pad), edge(big), edge(big), edge(pad), edge(pad),
            cells(tiles, 2, chips, block + pad), cells(tiles, chips, block + pad),
            cells(tiles, chips, block + pad), cells(tiles, chips, block + pad),
            pltpu.SemaphoreType.DMA((tiles, 7)), pltpu.SemaphoreType.DMA((tiles, 7)),
            pltpu.SemaphoreType.DMA((tiles,)), pltpu.SemaphoreType.DMA((tiles,)),
            pltpu.SemaphoreType.DMA((tiles, chips)), pltpu.SemaphoreType.DMA((tiles, chips)),
        ],
        compiler_params=pltpu.CompilerParams(
            dimension_semantics=("arbitrary",),
            vmem_limit_bytes=56 * 1024 * 1024,
            collective_id=0,
            has_side_effects=True,
        ),
        name="hyena_back",
    )(
        input_q, input_k, input_v, grad_out, input_q, input_k, input_v, grad_out,
        short_filters, long_filter, skip_gain[None], *mats,
    )
    return (back_q, back_k, back_v, grad_filt, grad_taps, grad_gain[0])


def solution(mesh):
    return jax.shard_map(
        body,
        mesh=mesh,
        in_specs=(
            P("seq", "ch"),
            P("seq", "ch"),
            P("seq", "ch"),
            P("seq", "ch"),
            P(None, None, "ch"),
            P(None, "ch"),
            P("ch"),
        ),
        out_specs=(
            P("seq", "ch"),
            P("seq", "ch"),
            P("seq", "ch"),
            P("seq", "ch"),
            P(None, None, "ch"),
            P("ch"),
        ),
        check_vma=False,
    )
```

```python
import functools

import jax
import jax.numpy as jnp
import numpy as np
from jax import lax
from jax.experimental import pallas as pl
from jax.experimental.pallas import tpu as pltpu
from jax.sharding import PartitionSpec as P

F32 = jnp.float32
BF16 = jnp.bfloat16
ROWS = 16


def transforms(span):
    freq = np.concatenate([np.arange(0, span, 2), np.arange(1, span, 2)]) + 0.5
    angle = np.pi * np.outer(freq, np.arange(span)) / span
    fwd = np.concatenate([np.cos(angle), -np.sin(angle)], 0)
    inv = fwd.T / span

    def halves(mat):
        mat = mat.astype(np.float32)
        high = mat.astype(jnp.bfloat16)
        low = (mat - high.astype(np.float32)).astype(jnp.bfloat16)
        return high, low

    fh, fl = halves(fwd)
    ih, il = halves(inv)
    return (
        np.concatenate([fh, fh, fl], 1),
        np.concatenate([ih, ih, il], 1),
        np.concatenate([np.eye(span)[::-1]] * 2, 1).astype(jnp.bfloat16),
    )


def split(value):
    high = value.astype(BF16)
    low = (value - high.astype(F32)).astype(BF16)
    return high, low


def down(window, by, rows):
    return pltpu.roll(window, by, 0)[8 : 8 + rows]


def up(window, by, rows):
    return pltpu.roll(window, rows + 8 - by, 0)[:rows]


def remote(src, dst, send, recv, target):
    return pltpu.make_async_remote_copy(
        src_ref=src,
        dst_ref=dst,
        send_sem=send,
        recv_sem=recv,
        device_id={"seq": target},
        device_id_type=pl.DeviceIdType.MESH,
    )


def kernel(
    size, length, span, ntap, pad,
    q_ref, k_ref, v_ref, g_ref, q_all, k_all, v_all, g_all,
    sf_ref, lf_ref, gain_ref, fh_ref, ih_ref, flip_ref,
    bq_ref, bk_ref, bv_ref, filt_ref, taps_ref, skip_ref,
    qx, kx, vx, gx, kf, vf, zf, gs, zw, gw, hw, acc, sx, gz, prod, part,
    kp_all, vp_all, qp_all, qn_all, gn_all, kn_all, vn_all,
    mine, theirs, chip, others,
    halo_send, halo_recv, pair_send, pair_recv, chip_send, chip_recv,
):
    width = q_ref.shape[1]
    half = span // 2
    nblk = length // span
    big = span + pad
    tile = pl.program_id(0)
    tiles = kp_all.shape[0]
    chips = size // 2
    block = span // size
    me = lax.axis_index("seq")
    core = lax.rem(me, 2)
    place = me // 2
    partner = me + 1 - 2 * core

    def to_next(t):
        cols = pl.ds(pl.multiple_of(t * width, width), width)
        target = lax.rem(me + 1, size)
        parts = ((k_all, big, kp_all), (v_all, big, vp_all), (q_all, pad, qp_all))
        return [
            remote(src.at[pl.ds(length - rows, rows), cols], dst.at[t], halo_send.at[t, j], halo_recv.at[t, j], target)
            for j, (src, rows, dst) in enumerate(parts)
        ]

    def to_prev(t):
        cols = pl.ds(pl.multiple_of(t * width, width), width)
        target = lax.rem(me + size - 1, size)
        parts = ((q_all, big, qn_all), (g_all, big, gn_all), (k_all, pad, kn_all), (v_all, pad, vn_all))
        return [
            remote(src.at[pl.ds(0, rows), cols], dst.at[t], halo_send.at[t, 3 + j], halo_recv.at[t, 3 + j], target)
            for j, (src, rows, dst) in enumerate(parts)
        ]

    def pair_copy(t):
        return remote(mine.at[t, 1 - core], theirs.at[t], pair_send.at[t], pair_recv.at[t], partner)

    def chip_copy(t, d):
        there = lax.rem(place + d, chips)
        return remote(chip.at[t, there], others.at[t, d], chip_send.at[t, d], chip_recv.at[t, d], there * 2 + core)

    @pl.when(tile == 0)
    def _():
        barrier = pltpu.get_barrier_semaphore()
        for d in range(1, size):
            pl.semaphore_signal(
                barrier, inc=1, device_id={"seq": lax.rem(me + d, size)}, device_id_type=pl.DeviceIdType.MESH
            )
        pl.semaphore_wait(barrier, size - 1)

        def send(t, _):
            @pl.when(me < size - 1)
            def _():
                for copy in to_next(t):
                    copy.start()

            @pl.when(me > 0)
            def _():
                for copy in to_prev(t):
                    copy.start()

            return 0

        lax.fori_loop(0, tiles, send, 0)

        @pl.when(me == 0)
        def _():
            for ref in (kp_all, vp_all, qp_all):
                ref[...] = jnp.zeros_like(ref)

        @pl.when(me == size - 1)
        def _():
            for ref in (qn_all, gn_all, kn_all, vn_all):
                ref[...] = jnp.zeros_like(ref)

    kp_ref, vp_ref, qp_ref = kp_all.at[tile], vp_all.at[tile], qp_all.at[tile]
    qn_ref, gn_ref, kn_ref, vn_ref = qn_all.at[tile], gn_all.at[tile], kn_all.at[tile], vn_all.at[tile]

    def join_chip(t):
        pair_copy(t).wait_recv()
        total = mine[t, core] + theirs[t]
        chip[t] = total
        others[t, 0] = mine[t, core, place] + theirs[t, place]
        for d in range(1, chips):
            chip_copy(t, d).start()

    kx[big : big + length] = k_ref[...].astype(F32)
    vx[big : big + length] = v_ref[...].astype(F32)
    qx[pad : pad + length] = q_ref[...].astype(F32)
    gx[:length] = g_ref[...].astype(F32)

    def taps(which):
        return [jnp.broadcast_to(sf_ref[which, i : i + 1, :], (ROWS, width)) for i in range(ntap)]

    def conv(ref, row, weights):
        window = ref[pl.ds(row - 8, ROWS + 8), :]
        total = weights[0] * window[8:]
        for i in range(1, ntap):
            total = total + weights[i] * down(window, i, ROWS)
        return total

    wk, wv, wq = taps(1), taps(2), taps(0)
    per = span // ROWS

    def make_z(c, _):
        row = pl.multiple_of(c * ROWS, ROWS)
        a = conv(kx, row + pad, wk)
        b = conv(vx, row + pad, wv)
        z = a * b
        kf[pl.ds(row, ROWS), :] = a
        vf[pl.ds(row, ROWS), :] = b
        zf[pl.ds(row, ROWS), :] = z
        return 0

    lax.fori_loop(per + 1, (span + length) // ROWS, make_z, 0, unroll=2)

    def make_g(c, _):
        row = pl.multiple_of(c * ROWS, ROWS)
        gs[pl.ds(row, ROWS), :] = gx[pl.ds(row, ROWS), :] * conv(qx, row + pad, wq)
        return 0

    lax.fori_loop(1, length // ROWS, make_g, 0, unroll=2)

    def forward(block, out):
        high, low = split(block)
        stack = jnp.concatenate([high, low, high], 0)
        out[...] = jnp.dot(fh_ref[...], stack, preferred_element_type=F32)

    def inverse(at, out):
        stack = jnp.concatenate([prod[at, 0], prod[at, 1], prod[at, 0]], 0)
        out[...] = jnp.dot(ih_ref[...], stack, preferred_element_type=F32)

    first = lax.broadcasted_iota(jnp.int32, (span, width), 0) == 0
    forward(lf_ref[...] + jnp.where(first, gain_ref[...], 0.0), hw)

    @pl.when(me > 0)
    def _():
        for copy in to_next(tile):
            copy.wait_recv()

    @pl.when(me < size - 1)
    def _():
        for copy in to_prev(tile):
            copy.wait_recv()

    kx[:big] = kp_ref[...].astype(F32)
    kx[big + length :] = kn_ref[...].astype(F32)
    vx[:big] = vp_ref[...].astype(F32)
    vx[big + length :] = vn_ref[...].astype(F32)
    qx[:pad] = qp_ref[...].astype(F32)
    qx[pad + length :] = qn_ref[...].astype(F32)
    gx[length:] = gn_ref[...].astype(F32)
    lax.fori_loop(0, per + 1, make_z, 0, unroll=2)
    make_z((span + length) // ROWS, 0)
    make_g(0, 0)
    lax.fori_loop(length // ROWS, (length + span + pad) // ROWS, make_g, 0, unroll=2)

    for b in range(nblk + 1):
        forward(zf[b * span : (b + 1) * span, :], zw.at[b])
        forward(gs[b * span : (b + 1) * span, :], gw.at[b])
    acc[...] = jnp.zeros_like(acc)

    @pl.when(tile > 0)
    def _():
        join_chip(tile - 1)

    for b in range(nblk):
        row = b * span
        for c in range(span // ROWS):
            sign = 1 if c * ROWS < half else -1
            re = slice(c * ROWS, (c + 1) * ROWS)
            im = slice(span + c * ROWS, span + (c + 1) * ROWS)
            hr, hi = hw[re], hw[im]
            if sign > 0:
                yr = zw[b + 1, re] - zw[b, im]
                yi = zw[b + 1, im] + zw[b, re]
            else:
                yr = zw[b + 1, re] + zw[b, im]
                yi = zw[b + 1, im] - zw[b, re]
            gr, gi = gw[b, re], gw[b, im]
            ph, plo = split(yr * hr - yi * hi)
            prod[2 * b, 0, re] = ph
            prod[2 * b, 1, re] = plo
            ph, plo = split(yr * hi + yi * hr)
            prod[2 * b, 0, im] = ph
            prod[2 * b, 1, im] = plo
            acc[re] += gr * yr + gi * yi
            acc[im] += gi * yr - gr * yi
        inverse(2 * b, sx.at[pl.ds(row, span)])
        for c in range(span // ROWS):
            sign = 1 if c * ROWS < half else -1
            re = slice(c * ROWS, (c + 1) * ROWS)
            im = slice(span + c * ROWS, span + (c + 1) * ROWS)
            hr, hi = hw[re], hw[im]
            if sign > 0:
                yr = gw[b, re] + gw[b + 1, im]
                yi = gw[b, im] - gw[b + 1, re]
            else:
                yr = gw[b, re] - gw[b + 1, im]
                yi = gw[b, im] + gw[b + 1, re]
            ph, plo = split(yr * hr + yi * hi)
            prod[2 * b + 1, 0, re] = ph
            prod[2 * b + 1, 1, re] = plo
            ph, plo = split(yi * hr - yr * hi)
            prod[2 * b + 1, 0, im] = ph
            prod[2 * b + 1, 1, im] = plo
        inverse(2 * b + 1, gz.at[pl.ds(row, span)])
    for c in range(span // ROWS):
        for start in (0, span):
            rows = slice(start + c * ROWS, start + (c + 1) * ROWS)
            ph, plo = split(acc[rows])
            prod[2 * nblk, 0, rows] = ph
            prod[2 * nblk, 1, rows] = plo
    inverse(2 * nblk, part)

    taps_h = lf_ref[...]
    back_h = jnp.dot(flip_ref[...], jnp.concatenate(split(taps_h), 0), preferred_element_type=F32)
    gain = gain_ref[...]
    line = lax.broadcasted_iota(jnp.int32, (8, width), 0)
    edge_s = jnp.zeros((8, width), F32)
    edge_z = jnp.zeros((8, width), F32)
    for i in range(ntap - 1):
        zrow = zf[length + span + i : length + span + i + 1, :]
        grow = gs[length + i : length + i + 1, :]
        win = zf[length + i + 1 : length + i + 1 + span, :]
        value = jnp.sum(win * back_h, axis=0, keepdims=True) + gain * zrow
        edge_s = jnp.where(line == i, value, edge_s)
        win = gs[length + i : length + i + span, :]
        value = jnp.sum(win * taps_h, axis=0, keepdims=True) + gain * grow
        edge_z = jnp.where(line == i, value, edge_z)
    eq = gx[length : length + 8] * edge_s
    ek = edge_z * vf[length + span : length + span + 8]
    ev = edge_z * kf[length + span : length + span + 8]

    def back(grad, after, weights, out_ref, row, own, sums):
        window = jnp.concatenate([grad, after], 0)
        total = weights[0] * grad
        new = [sums[0] + fold(grad * own)]
        for i in range(1, ntap):
            later = up(window, i, ROWS)
            total = total + weights[i] * later
            new.append(sums[i] + fold(later * own))
        out_ref[pl.ds(row, ROWS), :] = total.astype(BF16)
        return grad[:8], new

    def fold(value):
        total = value[:8]
        for r in range(8, ROWS, 8):
            total = total + value[r : r + 8]
        return total

    steps = length // ROWS

    def last(c, carry):
        after, sums = carry
        row = pl.multiple_of((steps - 1 - c) * ROWS, ROWS)
        gzc = gz[pl.ds(row, ROWS), :]
        gq = gx[pl.ds(row, ROWS), :] * sx[pl.ds(row, ROWS), :]
        gk = gzc * vf[pl.ds(row + span, ROWS), :]
        gv = gzc * kf[pl.ds(row + span, ROWS), :]
        aq, s0 = back(gq, after[0], wq, bq_ref, row, qx[pl.ds(row + pad, ROWS), :], sums[0])
        ak, s1 = back(gk, after[1], wk, bk_ref, row, kx[pl.ds(row + big, ROWS), :], sums[1])
        av, s2 = back(gv, after[2], wv, bv_ref, row, vx[pl.ds(row + big, ROWS), :], sums[2])
        return (aq, ak, av), (s0, s1, s2)

    zero = [jnp.zeros((8, width), F32) for _ in range(ntap)]
    _, sums = lax.fori_loop(0, steps, last, ((eq, ek, ev), (zero, zero, zero)), unroll=2)
    rows = [jnp.sum(sums[w][i], axis=0, keepdims=True) for w in range(3) for i in range(ntap)]
    rows.append(part[0:1, :])
    small = jnp.concatenate(rows + [jnp.zeros((pad - len(rows), width), F32)], 0)
    for d in range(size):
        mine[tile, d % 2, d // 2, :block] = part[d * block : (d + 1) * block]
        mine[tile, d % 2, d // 2, block:] = small
    pair_copy(tile).start()

    @pl.when(tile == tiles - 1)
    def _():
        join_chip(tiles - 1)

        def finish(t, _):
            cols = pl.ds(pl.multiple_of(t * width, width), width)

            @pl.when(me < size - 1)
            def _():
                for copy in to_next(t):
                    copy.wait_send()

            @pl.when(me > 0)
            def _():
                for copy in to_prev(t):
                    copy.wait_send()

            pair_copy(t).wait_send()
            for d in range(1, chips):
                chip_copy(t, d).wait_send()
                chip_copy(t, d).wait_recv()
            total = others[t, place]
            for z in range(1, chips):
                total = total + others[t, lax.rem(place + chips - z, chips)]
            filt_ref[:, cols] = total[:block]
            for w in range(3):
                for i in range(ntap):
                    at = block + w * ntap + i
                    taps_ref[w, i : i + 1, cols] = total[at : at + 1]
            at = block + 3 * ntap
            skip_ref[:, cols] = total[at : at + 1]
            return 0

        lax.fori_loop(0, tiles, finish, 0)


def body(input_q, input_k, input_v, grad_out, short_filters, long_filter, skip_gain):
    length, channels = input_q.shape
    ntap = short_filters.shape[1]
    span = long_filter.shape[0]
    pad = 16
    big = span + pad
    width = min(256, channels)
    mats = [jnp.asarray(m) for m in transforms(span)]
    nblk = length // span

    def tile(rows):
        return pl.BlockSpec((rows, width), lambda i: (0, i))

    def whole(mat):
        return pl.BlockSpec(mat.shape, lambda i: (0, 0))

    size = lax.axis_size("seq")
    tiles = channels // width
    chips = size // 2
    block = span // size
    cells = lambda *rows: pltpu.VMEM((*rows, width), F32)
    edge = lambda rows: pltpu.VMEM((tiles, rows, width), BF16)
    ext = length + big
    full = pl.BlockSpec(memory_space=pl.ANY)
    out = jax.ShapeDtypeStruct((length, channels), BF16)
    back_q, back_k, back_v, grad_filt, grad_taps, grad_gain = pl.pallas_call(
        functools.partial(kernel, size, length, span, ntap, pad),
        grid=(tiles,),
        out_shape=(
            out, out, out,
            jax.ShapeDtypeStruct((block, channels), F32),
            jax.ShapeDtypeStruct((3, ntap, channels), F32),
            jax.ShapeDtypeStruct((1, channels), F32),
        ),
        in_specs=[tile(length)] * 4
        + [full] * 4
        + [pl.BlockSpec((3, ntap, width), lambda i: (0, 0, i)), tile(span), tile(1)]
        + [whole(m) for m in mats],
        out_specs=(
            tile(length), tile(length), tile(length),
            pl.BlockSpec((block, channels), lambda i: (0, 0)),
            pl.BlockSpec((3, ntap, channels), lambda i: (0, 0, 0)),
            pl.BlockSpec((1, channels), lambda i: (0, 0)),
        ),
        scratch_shapes=[
            cells(ext + pad), cells(ext + pad), cells(ext + pad), cells(ext),
            cells(ext), cells(ext), cells(ext), cells(ext),
            cells(nblk + 1, 2 * span), cells(nblk + 1, 2 * span),
            cells(2 * span), cells(2 * span), cells(length), cells(length),
            pltpu.VMEM((2 * nblk + 1, 2, 2 * span, width), BF16), cells(span),
            edge(big), edge(big), edge(pad), edge(big), edge(big), edge(pad), edge(pad),
            cells(tiles, 2, chips, block + pad), cells(tiles, chips, block + pad),
            cells(tiles, chips, block + pad), cells(tiles, chips, block + pad),
            pltpu.SemaphoreType.DMA((tiles, 7)), pltpu.SemaphoreType.DMA((tiles, 7)),
            pltpu.SemaphoreType.DMA((tiles,)), pltpu.SemaphoreType.DMA((tiles,)),
            pltpu.SemaphoreType.DMA((tiles, chips)), pltpu.SemaphoreType.DMA((tiles, chips)),
        ],
        compiler_params=pltpu.CompilerParams(
            dimension_semantics=("arbitrary",),
            vmem_limit_bytes=56 * 1024 * 1024,
            collective_id=0,
            has_side_effects=True,
        ),
        name="hyena_back",
    )(
        input_q, input_k, input_v, grad_out, input_q, input_k, input_v, grad_out,
        short_filters, long_filter, skip_gain[None], *mats,
    )
    return (back_q, back_k, back_v, grad_filt, grad_taps, grad_gain[0])


def solution(mesh):
    return jax.shard_map(
        body,
        mesh=mesh,
        in_specs=(
            P("seq", "ch"),
            P("seq", "ch"),
            P("seq", "ch"),
            P("seq", "ch"),
            P(None, None, "ch"),
            P(None, "ch"),
            P("ch"),
        ),
        out_specs=(
            P("seq", "ch"),
            P("seq", "ch"),
            P("seq", "ch"),
            P("seq", "ch"),
            P(None, None, "ch"),
            P("ch"),
        ),
        check_vma=False,
    )
```
